32 devices in a mesh: cp: 16 (over z, y, core), tp: 2 (over x).
Axes of the slice: x: 2, y: 2, z: 4, core: 2. Of those that a mesh axis runs over, the one named last changes fastest.
Arguments:
- tokens: bfloat16 [8192, 4096], P('cp', 'tp'), may hold values from -40 to 40
- span_ids: int32 [16, 2], P('cp'), may hold values from 0 to 31, as said below
- positions: int32 [8192], P('cp'), may hold values from 0 to 4095, as said below
- q_weight: bfloat16 [4096, 1024], P(None, 'tp'), may hold values from -0.09375 to 0.09375
- k_weight: bfloat16 [4096, 256], P(None, 'tp'), may hold values from -0.09375 to 0.09375
- v_weight: bfloat16 [4096, 256], P(None, 'tp'), may hold values from -0.09375 to 0.09375
- o_weight: bfloat16 [1024, 4096], P('tp'), may hold values from -0.1875 to 0.1875
Outputs:
- attended: bfloat16 [8192, 4096], P('cp', 'tp')
The draws below stay inside these ranges and needn't reach their ends.
Inputs may be any that keep to these rules, and one draw needn't show every extreme that they name: `span_ids`: row r names the two spans held by index r of cp: a span c and the span 32 - 1 - c, in either order; every span is named once. Span c covers the places c * (256) to (c + 1) * 256 - 1 of the sequence. `positions`: along the sequence (in the order of places given by span_ids) documents are runs of consecutive tokens; a position is 0 at a document's first token and rises by one up to its last, and the first place of the sequence has position 0.
All inputs are finite; a program needn't handle non-finite values.
Results may differ from the reference program's by a relative error of at most 0.014.
The reference program's roundings to bfloat16 on the way count: a program that leaves them out, or rounds other values in their place, can miss the bound.
Values may be sent and summed in bfloat16 or wider, within the bound.
No kernel may reach another device: no remote copies, remote signals or barrier semaphores. Data moves between devices by JAX's collectives and lax.ppermute only.
A program may use at most 64 MiB of HBM per device.

```python
import jax
import jax.numpy as jnp
from jax import lax

D = 4096
HD = 128
HEADS_DEV = 4
TOK_DEV = 512
HEADS = 8
KV_HEADS = 2
TOKENS = 8192
N_CP = 16
N_TP = 2


def paired_table(key):
    rank_count = TOKENS // TOK_DEV
    shuffled = jax.random.permutation(jax.random.fold_in(key, 11), rank_count).astype(jnp.int32)
    swapped = jax.random.randint(jax.random.fold_in(key, 12), (rank_count,), 0, 2)
    low_span = shuffled
    high_span = (2 * rank_count - 1 - shuffled).astype(jnp.int32)
    first_span = jnp.where(swapped == 1, high_span, low_span)
    second_span = jnp.where(swapped == 1, low_span, high_span)
    return jnp.stack([first_span, second_span], axis=1).astype(jnp.int32)


def draw_span_ids(key, part):
    return paired_table(key)


def draw_positions(key, part):
    span_table = paired_table(key)
    half_rows = TOK_DEV // 2
    half_tokens = TOKENS // 2
    token_index = jnp.arange(TOKENS, dtype=jnp.int32)
    start_marks = jax.random.randint(jax.random.fold_in(key, 13), (TOKENS,), 0, max(TOKENS // 8, 2))
    marked = (start_marks == 0) & (token_index > half_tokens)
    starts = jnp.where(marked | (token_index == 0) | (token_index == half_tokens), token_index, 0)
    latest = lax.cummax(starts, axis=0)
    sequence_pos = (token_index - latest).astype(jnp.int32)
    offsets = jnp.arange(half_rows, dtype=jnp.int32)
    layout_index = (span_table[:, :, None] * half_rows + offsets[None, None, :]).reshape(TOKENS)
    return sequence_pos[layout_index].astype(jnp.int32)


def draw_tokens(key, part):
    normal_draw = jax.random.normal(jax.random.fold_in(key, 21), (TOKENS, D), jnp.float32)
    return jnp.clip(normal_draw, -40.0, 40.0).astype(jnp.bfloat16)


def block_scale(key, dims, cuts, smallest, largest):
    gain, own = 1.0, jax.random.fold_in(key, 6)
    for axis_at, blocks in cuts:
        steps = jnp.exp(jax.random.uniform(jax.random.fold_in(own, axis_at), (blocks,), jnp.float32, smallest / len(cuts), largest / len(cuts)))
        gain = gain * jnp.repeat(steps, dims[axis_at] // blocks).reshape([-1 if axis == axis_at else 1 for axis in range(len(dims))])
    return gain


def scatter_about(rng, dims, scale, reach, split=(), kind=jnp.bfloat16):
    factor_of = block_scale(rng, dims, split, -0.22, 0.18) if split else 1.0
    array = jax.random.normal(rng, dims, jnp.float32) * scale * factor_of
    return jnp.minimum(jnp.maximum(array, -reach), reach).astype(kind)


def setup_inputs(seed: int = 0) -> dict:
    streams_of = jax.random.split(jax.random.key(seed), 8)
    return {
        "tokens": draw_tokens(jax.random.fold_in(streams_of[7], 71), 0),
        "span_ids": draw_span_ids(jax.random.fold_in(streams_of[7], 71), 0),
        "positions": draw_positions(jax.random.fold_in(streams_of[7], 71), 0),
        "q_weight": scatter_about(streams_of[3], (D, HEADS * HD), D ** -0.5, 0.09375, ((1, 2),)),
        "k_weight": scatter_about(streams_of[4], (D, KV_HEADS * HD), D ** -0.5, 0.09375, ((1, 2),)),
        "v_weight": scatter_about(streams_of[5], (D, KV_HEADS * HD), D ** -0.5, 0.09375, ((1, 2),)),
        "o_weight": scatter_about(streams_of[6], (HEADS * HD, D), (HEADS * HD) ** -0.5, 0.1875, ((0, 2),)),
    }


theta_base = 500000.0


def rotate(vectors, positions):
    half_size = vectors.shape[-1] // 2
    exponent = jnp.arange(half_size, dtype=jnp.float32) * (2.0 / vectors.shape[-1])
    inverse_freq = theta_base ** (-exponent)
    angles = positions.astype(jnp.float32)[:, None] * inverse_freq[None, :]
    cosine = jnp.cos(angles)[:, None, :]
    sine_part = jnp.sin(angles)[:, None, :]
    lower_half = vectors[..., :half_size]
    upper_half = vectors[..., half_size:]
    return jnp.concatenate([lower_half * cosine - upper_half * sine_part, upper_half * cosine + lower_half * sine_part], axis=-1)


def reference(tokens, span_ids, positions, q_weight, k_weight, v_weight, o_weight):
    half_rows = TOK_DEV // 2
    scale_factor = HD ** -0.5
    queries = jnp.dot(tokens, q_weight, preferred_element_type=jnp.float32).reshape(TOKENS, HEADS, HD)
    keys_all = jnp.dot(tokens, k_weight, preferred_element_type=jnp.float32).reshape(TOKENS, KV_HEADS, HD)
    values_all = jnp.dot(tokens, v_weight, preferred_element_type=jnp.float32).astype(jnp.bfloat16).reshape(TOKENS, KV_HEADS, HD)
    queries = rotate(queries, positions).astype(jnp.bfloat16)
    keys_all = rotate(keys_all, positions).astype(jnp.bfloat16)
    offsets = jnp.arange(half_rows, dtype=jnp.int32)
    global_index = (span_ids[:, :, None] * half_rows + offsets[None, None, :]).reshape(TOKENS).astype(jnp.int32)
    doc_start = (global_index - positions).astype(jnp.int32)
    head_keys = jnp.transpose(keys_all, (1, 0, 2))
    head_values = jnp.transpose(values_all, (1, 0, 2))

    def one_block(inputs):
        block_queries, block_index, block_start = inputs
        grouped = jnp.transpose(block_queries.reshape(TOK_DEV, KV_HEADS, HEADS_DEV, HD), (1, 2, 0, 3))
        visible = (global_index[None, :] <= block_index[:, None]) & (global_index[None, :] >= block_start[:, None])

        def one_head(head_inputs):
            group_queries, keys_one, values_one = head_inputs
            scores = jnp.einsum("grd,kd->grk", group_queries.astype(jnp.float32), keys_one.astype(jnp.float32)) * scale_factor
            scores = jnp.where(visible[None], scores, -jnp.inf)
            row_max = jnp.max(scores, axis=-1, keepdims=True)
            weights = jnp.exp(scores - row_max)
            weight_sum = jnp.sum(weights, axis=-1, keepdims=True)
            rounded = lax.optimization_barrier(weights.astype(jnp.bfloat16)).astype(jnp.float32)
            mixture = jnp.einsum("grk,kd->grd", rounded, values_one.astype(jnp.float32))
            return mixture / weight_sum

        heads_out = lax.map(one_head, (grouped, head_keys, head_values))
        return jnp.transpose(heads_out, (2, 0, 1, 3)).reshape(TOK_DEV, HEADS * HD).astype(jnp.bfloat16)

    attended = lax.map(one_block, (queries.reshape(N_CP, TOK_DEV, HEADS, HD), global_index.reshape(N_CP, TOK_DEV), doc_start.reshape(N_CP, TOK_DEV)))
    attended = attended.reshape(TOKENS, N_TP, HEADS_DEV * HD)
    out_weight = o_weight.reshape(N_TP, HEADS_DEV * HD, D)
    summed = jnp.zeros((TOKENS, D), jnp.float32)
    for tp_rank in range(N_TP):
        partial_sum = jnp.dot(attended[:, tp_rank], out_weight[tp_rank], preferred_element_type=jnp.float32)
        summed = summed + lax.optimization_barrier(partial_sum.astype(jnp.bfloat16)).astype(jnp.float32)
    return summed.astype(jnp.bfloat16)
```

```python
from functools import partial

import jax
import jax.numpy as jnp
from jax import lax
from jax.experimental import pallas as pl
from jax.experimental.pallas import tpu as pltpu
from jax.sharding import PartitionSpec as P

HD = 128
TILE = 128
theta_base = 500000.0
floor_score = -1e30
far_key = 1 << 30
VMEM_LIMIT = 48 * 1024 * 1024


def levels_of(count):
    core = 2 if count % 2 == 0 else 1
    rest = count // core
    outer = 4 if rest % 4 == 0 else rest
    return outer, rest // outer, core


def cp_shift(block, levels, steps):
    zn, yn, cn = levels
    route = []
    for z in range(zn):
        for y in range(yn):
            for c in range(cn):
                to = (((z + steps[0]) % zn) * yn + (y + steps[1]) % yn) * cn + (c + steps[2]) % cn
                route.append(((z * yn + y) * cn + c, to))
    return lax.ppermute(block, "cp", route)


def gather_blocks(block, levels):
    zn, yn, cn = levels
    along_z = [block] + [cp_shift(block, levels, (a, 0, 0)) for a in range(1, zn)]
    chips = []
    for a in range(zn):
        chips += [along_z[a]] + [cp_shift(along_z[a], levels, (0, b, 0)) for b in range(1, yn)]
    out = list(chips)
    for c in range(1, cn):
        out += [cp_shift(chip, levels, (0, 0, c)) for chip in chips]
    return jnp.stack(out)


def tp_shift(block, count, distance):
    return lax.ppermute(block, "tp", [(i, (i + distance) % count) for i in range(count)])


def angle_tables(positions):
    half = HD // 2
    exponent = jnp.arange(half, dtype=jnp.float32) * (2.0 / HD)
    inverse_freq = theta_base ** (-exponent)
    angles = positions.astype(jnp.float32)[:, None] * inverse_freq[None, :]
    cosine, sine = jnp.cos(angles), jnp.sin(angles)
    return (
        jnp.concatenate([cosine, cosine], axis=1),
        jnp.concatenate([-sine, sine], axis=1),
    )


def own_kernel(where, tok, wq, wk, wv, out):
    @pl.when(pl.program_id(0) == 0)
    def _():
        out[...] = jnp.zeros_like(out)

    nq, nk = wq.shape[1], wk.shape[1]
    x = tok[...]
    out[:, :nq] += jnp.dot(x, wq[...], preferred_element_type=jnp.float32)
    out[:, nq : nq + nk] += jnp.dot(x, wk[...], preferred_element_type=jnp.float32)
    out[:, nq + nk :] += jnp.dot(x, wv[...], preferred_element_type=jnp.float32)


def own_part(tokens, weights, tp_index):
    rows, width = tokens.shape
    step = min(512, width)
    steps = width // step
    cols = [w.shape[1] for w in weights]
    total = sum(cols)
    return pl.pallas_call(
        own_kernel,
        name="own_part",
        grid_spec=pltpu.PrefetchScalarGridSpec(
            num_scalar_prefetch=1,
            grid=(steps,),
            in_specs=[pl.BlockSpec((rows, step), lambda k, w: (0, k))]
            + [pl.BlockSpec((step, c), lambda k, w: (w[0] * steps + k, 0)) for c in cols],
            out_specs=pl.BlockSpec((rows, total), lambda k, w: (0, 0)),
        ),
        out_shape=jax.ShapeDtypeStruct((rows, total), jnp.float32),
        cost_estimate=pl.CostEstimate(
            flops=2 * rows * width * total,
            bytes_accessed=2 * width * (rows + total) + 4 * rows * total,
            transcendentals=0,
        ),
        compiler_params=pltpu.CompilerParams(vmem_limit_bytes=VMEM_LIMIT),
    )(tp_index, tokens, *weights)


def project_kernel(where, tok, wq, wk, wv, own, cosine, sine, q_out, kv_out, total):
    d, k = pl.program_id(0), pl.program_id(1)

    @pl.when((d == 0) & (k == 0))
    def _():
        total[...] = own[...]

    nq, nk = wq.shape[1], wk.shape[1]
    x = tok[0]
    total[:, :nq] += jnp.dot(x, wq[...], preferred_element_type=jnp.float32)
    total[:, nq : nq + nk] += jnp.dot(x, wk[...], preferred_element_type=jnp.float32)
    total[:, nq + nk :] += jnp.dot(x, wv[...], preferred_element_type=jnp.float32)

    @pl.when((d == pl.num_programs(0) - 1) & (k == pl.num_programs(1) - 1))
    def _():
        cos, sin = cosine[...], sine[...]

        def rotated(at):
            x = total[:, at : at + HD]
            return (x * cos + pltpu.roll(x, HD // 2, 1) * sin).astype(jnp.bfloat16)

        for h in range(q_out.shape[0]):
            q_out[h] = rotated(h * HD)
        keys = rotated(nq)
        values = total[:, nq + nk :]
        for t in range(kv_out.shape[0]):
            rows = slice(t * TILE, (t + 1) * TILE)
            kv_out[t, 0] = keys[rows]
            kv_out[t, 1] = values[rows].T.astype(jnp.bfloat16)


def project(received, weights, own, cosine, sine, tp_index, row_block, tp_count):
    others, rows, width = received.shape
    step = min(512, width)
    steps = width // step
    cols = [w.shape[1] for w in weights]
    total = sum(cols)
    where = jnp.concatenate([tp_index, row_block])

    def weight_block(d, k, w):
        return (lax.rem(w[0] + tp_count - 1 - d, tp_count) * steps + k, 0)

    def row_spec(width_of):
        return pl.BlockSpec((rows, width_of), lambda d, k, w: (w[1], 0))

    heads = cols[0] // HD
    return pl.pallas_call(
        project_kernel,
        name="project",
        grid_spec=pltpu.PrefetchScalarGridSpec(
            num_scalar_prefetch=1,
            grid=(others, steps),
            in_specs=[pl.BlockSpec((1, rows, step), lambda d, k, w: (d, 0, k))]
            + [pl.BlockSpec((step, c), weight_block) for c in cols]
            + [row_spec(total), row_spec(HD), row_spec(HD)],
            out_specs=[
                pl.BlockSpec((heads, rows, HD), lambda d, k, w: (0, 0, 0)),
                pl.BlockSpec((rows // TILE, 2, TILE, HD), lambda d, k, w: (0, 0, 0, 0)),
            ],
            scratch_shapes=[pltpu.VMEM((rows, total), jnp.float32)],
        ),
        out_shape=[
            jax.ShapeDtypeStruct((heads, rows, HD), jnp.bfloat16),
            jax.ShapeDtypeStruct((rows // TILE, 2, TILE, HD), jnp.bfloat16),
        ],
        cost_estimate=pl.CostEstimate(
            flops=2 * others * rows * width * total,
            bytes_accessed=2 * others * width * (rows + total) + 4 * rows * total,
            transcendentals=0,
        ),
        compiler_params=pltpu.CompilerParams(vmem_limit_bytes=VMEM_LIMIT),
    )(where, received, *weights, own, cosine, sine)


def attend_kernel(
    table, me, starts, *refs, levels, q_rows, part, key_sets, has_state, final
):
    refs = list(refs)
    s_row = refs.pop(0)
    q_refs = [refs.pop(0) for _ in q_rows]
    kv_refs = [refs.pop(0) for _ in key_sets]
    state_in = [refs.pop(0) for _ in range(3)] if has_state else None
    if final:
        out = refs.pop(0)
        m_ref, l_ref, acc_ref = refs[:3]
        list_t, list_s = refs[3:]
    else:
        m_ref, l_ref, acc_ref = refs[:3]
        list_t, list_s = refs[3:]

    zn, yn, cn = levels
    span_rows = s_row.shape[1]
    width = 2 * TILE
    factor = HD**-0.5 * 1.4426950408889634

    def span_start(device, which):
        first, second = table[2 * device], table[2 * device + 1]
        span = jnp.minimum(first, second) if which == 0 else jnp.maximum(first, second)
        return span * span_rows

    mine = me[0]
    my_c = lax.rem(mine, cn)
    my_y = lax.rem(lax.div(mine, cn), yn)
    my_z = lax.div(mine, cn * yn)
    g0 = span_start(mine, part)
    s_first = starts[part * span_rows]
    s_last = starts[part * span_rows + span_rows - 1]

    groups = []
    lane = lax.broadcasted_iota(jnp.int32, (1, width), 1)
    first_row = 0
    for ref, rows in zip(q_refs, q_rows):
        per_head = rows
        places = g0 + first_row + lax.rem(lane, per_head)
        begin = s_row[part : part + 1, first_row : first_row + rows]
        if rows < width:
            begin = jnp.concatenate([begin] * (width // rows), axis=1)
        for at in range(ref.shape[0] // width):
            groups.append((ref, at * width, places, begin, first_row, rows))
        first_row += rows

    if has_state:
        m_ref[...] = state_in[0][...]
        l_ref[...] = state_in[1][...]
        acc_ref[...] = state_in[2][...]
    else:
        m_ref[...] = jnp.full_like(m_ref, floor_score)
        l_ref[...] = jnp.zeros_like(l_ref)
        acc_ref[...] = jnp.zeros_like(acc_ref)

    for kv, (key_part, key_row, per_block) in zip(kv_refs, key_sets):
        tiles = kv.shape[0]

        def add_tile(t, count):
            block = lax.div(t, per_block)
            c = lax.div(block, zn * yn)
            a = lax.div(lax.rem(block, zn * yn), yn)
            b = lax.rem(block, yn)
            z = lax.rem(my_z + zn - a, zn)
            y = lax.rem(my_y + yn - b, yn)
            c = lax.rem(my_c + cn - c, cn)
            first = span_start((z * yn + y) * cn + c, key_part)
            first = first + key_row + lax.rem(t, per_block) * TILE
            list_t[count] = t
            list_s[count] = first
            needed = (first < g0 + span_rows) & (first + TILE > s_first)
            return count + needed.astype(jnp.int32)

        count = lax.fori_loop(0, tiles, add_tile, jnp.int32(0))
        list_t[count] = 0
        list_s[count] = far_key

        def visit(i, masked):
            t0, t1 = list_t[2 * i], list_t[2 * i + 1]
            keys = jnp.concatenate([kv[t0, 0], kv[t1, 0]], axis=0)
            values = jnp.concatenate([kv[t0, 1], kv[t1, 1]], axis=1)
            if masked:
                row = lax.broadcasted_iota(jnp.int32, (2 * TILE, 1), 0)
                key_at = row + jnp.where(row < TILE, list_s[2 * i], list_s[2 * i + 1] - TILE)
            for n, (ref, at, places, begin, _, _) in enumerate(groups):
                cols = slice(n * width, (n + 1) * width)
                scores = lax.dot_general(
                    keys, ref[at : at + width, :], (((1,), (1,)), ((), ())),
                    preferred_element_type=jnp.float32,
                )
                if masked:
                    seen = (key_at <= places) & (key_at >= begin)
                    scores = jnp.where(seen, scores, floor_score)
                old = m_ref[0:1, cols]
                new = jnp.maximum(old, jnp.max(scores, axis=0, keepdims=True))
                e = jnp.exp2((scores - new) * factor)
                shrink = jnp.exp2((old - new) * factor)
                m_ref[0:1, cols] = new
                l_ref[0:1, cols] = l_ref[0:1, cols] * shrink + jnp.sum(e, axis=0, keepdims=True)
                acc_ref[:, cols] = acc_ref[:, cols] * shrink + jnp.dot(
                    values, e.astype(jnp.bfloat16), preferred_element_type=jnp.float32
                )

        def step(i, carry):
            f0, f1 = list_s[2 * i], list_s[2 * i + 1]
            whole = (jnp.maximum(f0, f1) + TILE - 1 <= g0) & (jnp.minimum(f0, f1) >= s_last)
            pl.when(whole)(lambda: visit(i, False))
            pl.when(jnp.logical_not(whole))(lambda: visit(i, True))
            return carry

        lax.fori_loop(0, lax.div(count + 1, 2), step, 0)

    if final:
        for n, (_, at, _, _, first_row, rows) in enumerate(groups):
            cols = slice(n * width, (n + 1) * width)
            mixed = (acc_ref[:, cols] / l_ref[0:1, cols]).T.astype(jnp.bfloat16)
            for piece in range(width // rows):
                head = at // rows + piece
                out[first_row : first_row + rows, head * HD : (head + 1) * HD] = mixed[
                    piece * rows : (piece + 1) * rows
                ]


def attend(table, me, s_rows, queries, key_arrays, key_sets, part, levels, state, final):
    heads = queries[0].shape[0]
    q_rows = tuple(q.shape[1] for q in queries)
    flat = [q.reshape(heads * q.shape[1], HD) for q in queries]
    columns = heads * sum(q_rows)
    tiles = sum(k.shape[0] for k in key_arrays)
    most = max(k.shape[0] for k in key_arrays)
    state_shapes = [
        jax.ShapeDtypeStruct((8, columns), jnp.float32),
        jax.ShapeDtypeStruct((8, columns), jnp.float32),
        jax.ShapeDtypeStruct((HD, columns), jnp.float32),
    ]
    whole = pl.BlockSpec(memory_space=pltpu.VMEM)
    operands = [s_rows] + flat + list(key_arrays) + (list(state) if state else [])
    lists = [pltpu.SMEM((most + 2,), jnp.int32), pltpu.SMEM((most + 2,), jnp.int32)]
    scratch = [pltpu.VMEM(s.shape, s.dtype) for s in state_shapes] if final else []
    if final:
        out_shape = jax.ShapeDtypeStruct((sum(q_rows), heads * HD), jnp.bfloat16)
        out_specs = whole
    else:
        out_shape = state_shapes
        out_specs = [whole] * 3
    work = columns * tiles * TILE
    return pl.pallas_call(
        partial(
            attend_kernel, levels=levels, q_rows=q_rows, part=part, key_sets=tuple(key_sets),
            has_state=bool(state), final=final,
        ),
        name="attend",
        grid_spec=pltpu.PrefetchScalarGridSpec(
            num_scalar_prefetch=3,
            grid=(),
            in_specs=[whole] * len(operands),
            out_specs=out_specs,
            scratch_shapes=scratch + lists,
        ),
        out_shape=out_shape,
        cost_estimate=pl.CostEstimate(
            flops=2 * HD * work, bytes_accessed=tiles * 4 * TILE * HD, transcendentals=work // 2
        ),
        compiler_params=pltpu.CompilerParams(vmem_limit_bytes=VMEM_LIMIT),
    )(table, me, s_rows.reshape(-1), *operands)


def output_kernel(where, attn, other, w_own, w_same, w_swap, *refs):
    out = refs[-1]
    half = w_same.shape[1]
    mine = jnp.dot(attn[...], w_own[...], preferred_element_type=jnp.float32)
    total = mine.astype(jnp.bfloat16).astype(jnp.float32)
    at_same = pl.multiple_of(where[2] * half, half)
    at_swap = pl.multiple_of((1 - where[2]) * half, half)
    for d in range(other.shape[0]):
        part = jnp.dot(
            other[d, :, pl.ds(at_same, half)], w_same[d], preferred_element_type=jnp.float32
        ) + jnp.dot(
            other[d, :, pl.ds(at_swap, half)], w_swap[d], preferred_element_type=jnp.float32
        )
        total = total + part.astype(jnp.bfloat16).astype(jnp.float32)
    out[...] = total.astype(jnp.bfloat16)


def project_out(where, attn, other, o_weight, o_same, o_swap, rows_all, before):
    rows, depth = attn.shape
    others, half, width = o_same.shape
    step = min(512, width)
    steps = width // step
    whole = [] if before is None else [before]
    return pl.pallas_call(
        output_kernel,
        name="project_out",
        grid_spec=pltpu.PrefetchScalarGridSpec(
            num_scalar_prefetch=1,
            grid=(steps,),
            in_specs=[
                pl.BlockSpec((rows, depth), lambda j, w: (0, 0)),
                pl.BlockSpec((others, rows, depth), lambda j, w: (0, 0, 0)),
                pl.BlockSpec((depth, step), lambda j, w: (0, w[1] * steps + j)),
                pl.BlockSpec((others, half, step), lambda j, w: (0, 0, j)),
                pl.BlockSpec((others, half, step), lambda j, w: (0, 0, j)),
            ]
            + [pl.BlockSpec(memory_space=pl.ANY)] * len(whole),
            out_specs=pl.BlockSpec((rows, step), lambda j, w: (w[0], j)),
        ),
        out_shape=jax.ShapeDtypeStruct((rows_all, width), jnp.bfloat16),
        input_output_aliases={6: 0} if whole else {},
        cost_estimate=pl.CostEstimate(
            flops=2 * rows * depth * width * (others + 1),
            bytes_accessed=2 * width * (depth * (others + 1) + rows),
            transcendentals=0,
        ),
        compiler_params=pltpu.CompilerParams(vmem_limit_bytes=VMEM_LIMIT),
    )(where, attn, other, o_weight, o_same, o_swap, *whole)


def per_device(tokens, span_ids, positions, q_weight, k_weight, v_weight, o_weight):
    rows, width = tokens.shape
    span_rows = rows // 2
    half_span = span_rows // 2
    cp_count, tp_count = lax.axis_size("cp"), lax.axis_size("tp")
    levels = levels_of(cp_count)
    weights = (q_weight, k_weight, v_weight)
    tp_index = lax.axis_index("tp").astype(jnp.int32).reshape(1)
    cp_index = lax.axis_index("cp").astype(jnp.int32).reshape(1)
    core = lax.rem(cp_index, levels[2])

    flip = (span_ids[0, 0] > span_ids[0, 1]).astype(jnp.int32)
    spots = (flip, 1 - flip)
    chunks = ((0, 0, span_rows), (1, 0, half_span), (1, half_span, span_rows - half_span))

    table = lax.all_gather(span_ids, "cp", axis=0, tiled=True).reshape(-1)

    received = []
    for part, first, count in chunks:
        piece = lax.dynamic_slice_in_dim(tokens, spots[part] * span_rows + first, count)
        received.append(
            jnp.stack([tp_shift(piece, tp_count, d) for d in range(1, tp_count)])
        )

    own = own_part(tokens, weights, tp_index)
    cosine, sine = angle_tables(positions)
    low_high = jnp.sort(span_ids[0])
    halves = positions.reshape(2, span_rows)
    halves = jnp.where(flip == 1, halves[::-1], halves)
    s_rows = low_high[:, None] * span_rows + jnp.arange(span_rows, dtype=jnp.int32) - halves

    queries, gathered, key_sets = [], [], []
    for (part, first, count), block in zip(chunks, received):
        row_block = (spots[part] * (span_rows // count) + first // count).reshape(1)
        q, kv = project(block, weights, own, cosine, sine, tp_index, row_block, tp_count)
        queries.append(q)
        blocks = gather_blocks(kv, levels)
        gathered.append(blocks.reshape((-1,) + blocks.shape[2:]))
        key_sets.append((part, first, kv.shape[0]))

    half_depth = o_weight.shape[0] // 2
    gate, _ = lax.optimization_barrier((o_weight, received[-1]))
    same = []
    for d in range(1, tp_count):
        to = lax.rem(tp_index[0] + d, tp_count)
        piece = lax.dynamic_slice(
            gate, (core[0] * half_depth, to * width), (half_depth, width)
        )
        same.append(tp_shift(piece, tp_count, d))
    o_same = jnp.stack(same)
    o_swap = cp_shift(o_same, levels, (0, 0, 1))

    low = attend(
        table, cp_index, s_rows, queries[:1], gathered[:1], key_sets[:1], 0, levels, None, True
    )
    low_other = jnp.stack([tp_shift(low, tp_count, d) for d in range(1, tp_count)])
    state = attend(
        table, cp_index, s_rows, queries[1:], gathered[:2], key_sets[:2], 1, levels, None, False
    )
    high = attend(
        table, cp_index, s_rows, queries[1:], gathered[2:], key_sets[2:], 1, levels, state, True
    )
    high_other = jnp.stack([tp_shift(high, tp_count, d) for d in range(1, tp_count)])

    def place(part):
        return jnp.concatenate([spots[part].reshape(1), tp_index, core])

    out = project_out(place(0), low, low_other, o_weight, o_same, o_swap, rows, None)
    return project_out(place(1), high, high_other, o_weight, o_same, o_swap, rows, out)


def solution(mesh):
    in_specs = (
        P("cp", "tp"),
        P("cp", None),
        P("cp"),
        P(None, "tp"),
        P(None, "tp"),
        P(None, "tp"),
        P("tp", None),
    )
    return jax.shard_map(
        per_device, mesh=mesh, in_specs=in_specs, out_specs=P("cp", "tp"), check_vma=False
    )
```
